32 devices in a mesh: rep: 1 (over z), r: 4 (over y), s: 8 (over x, core).
Axes of the slice: x: 4, y: 4, z: 1, core: 2. Of those that a mesh axis runs over, the one named last changes fastest.
The devices are a block of a 4x4x8 slice.
Arguments:
- x: bfloat16 [32, 2048, 1024], P(('rep', 'r', 's'))
- dy: bfloat16 [32, 2048, 1024], P(('rep', 'r', 's'))
- w_gate: bfloat16 [2, 1024, 2816], P(None, 's')
- w_up: bfloat16 [2, 1024, 2816], P(None, 's')
- w_down: bfloat16 [2, 2816, 1024], P(None, 's')
- m_w_gate: float32 [2, 1024, 2816], P(None, 's')
- m_w_up: float32 [2, 1024, 2816], P(None, 's')
- m_w_down: float32 [2, 2816, 1024], P(None, 's')
- v_w_gate: float32 [2, 1024, 2816], P(None, 's')
- v_w_up: float32 [2, 1024, 2816], P(None, 's')
- v_w_down: float32 [2, 2816, 1024], P(None, 's')
Outputs:
- output 1: bfloat16 [2, 1024, 2816], P('rep', 's')
- output 2: bfloat16 [2, 1024, 2816], P('rep', 's')
- output 3: bfloat16 [2, 2816, 1024], P('rep', 's')
- output 4: float32 [2, 1024, 2816], P('rep', 's')
- output 5: float32 [2, 1024, 2816], P('rep', 's')
- output 6: float32 [2, 2816, 1024], P('rep', 's')
- output 7: float32 [2, 1024, 2816], P('rep', 's')
- output 8: float32 [2, 1024, 2816], P('rep', 's')
- output 9: float32 [2, 2816, 1024], P('rep', 's')
All inputs are finite; a program needn't handle non-finite values.
Results may differ from the reference program's by a relative error of at most 0.02.
Values are sent between devices in bfloat16 or wider.
A program may use at most 768 MiB of HBM per device.

```python
import jax
import jax.numpy as jnp
from jax import lax

SEQUENCES = 32
TOKENS = 2048
D = 1024
FF = 2816
LAYERS = 2
NAMES = ("w_gate", "w_up", "w_down")
SHAPES = {"w_gate": (LAYERS, D, FF), "w_up": (LAYERS, D, FF), "w_down": (LAYERS, FF, D)}


def bump(key, n, height):
    away = (jnp.arange(n, dtype=jnp.int32) - jax.random.randint(key, (), 0, n, jnp.int32)) % n
    return jnp.where(away < n // 8, height, 1.0)


def together(key, own, strength):
    shared = jax.random.normal(key, own.shape[1:], jnp.float32)
    return (own + strength * shared) * lax.rsqrt(1 + strength * strength)


def setup_inputs(seed: int = 0, part: int = 0) -> dict:
    kx, kdy, ka, kb, kz, kf, kh, kl, *keys = jax.random.split(jax.random.key(seed), 8 + 3 * len(NAMES))
    kx, kdy, ka, kb = (jax.random.fold_in(k, part) for k in (kx, kdy, ka, kb))
    kw, km, kv = (keys[i::3] for i in range(3))
    shape = (SEQUENCES, TOKENS, D)
    much_x, much_dy = jax.random.uniform(kz, (2,), jnp.float32, 0.0, 1.0)
    loud = 2.0 ** jax.random.uniform(jax.random.fold_in(kz, 1), (), jnp.float32, -1.0, 2.0)
    layers = 2.0 ** jax.random.uniform(kl, (LAYERS, 1, 1), jnp.float32, -1.0, 1.0)
    x = together(ka, jax.random.normal(kx, shape, jnp.float32), much_x) * bump(kf, D, 4.0)
    dy = together(kb, jax.random.normal(kdy, shape, jnp.float32), much_dy)
    drawn = {"x": x.astype(jnp.bfloat16), "dy": (loud * dy * (SEQUENCES * TOKENS) ** -0.5).astype(jnp.bfloat16)}
    for key, name in zip(kw, NAMES, strict=True):
        w = jax.random.normal(key, SHAPES[name], jnp.float32) * SHAPES[name][1] ** -0.5
        drawn[name] = (w * {"w_gate": 1.0, "w_up": bump(kh, FF, 4.0), "w_down": layers}[name]).astype(jnp.bfloat16)
    for key, name in zip(km, NAMES, strict=True):
        drawn[f"m_{name}"] = 0.1 * jax.random.normal(key, SHAPES[name], jnp.float32)
    for key, name in zip(kv, NAMES, strict=True):
        drawn[f"v_{name}"] = jax.random.uniform(key, SHAPES[name], jnp.float32, 0.005, 0.015)
    return drawn


def matmul(a, w):
    return jnp.dot(a, w, preferred_element_type=jnp.float32).astype(jnp.bfloat16)


def normed(h):
    wide = h.astype(jnp.float32)
    scale = lax.rsqrt(jnp.mean(wide**2, -1, keepdims=True) + 1e-6)
    return (wide * scale).astype(jnp.bfloat16)


def layer(h, w):
    a = normed(h)
    gate = jnp.dot(a, w["w_gate"], preferred_element_type=jnp.float32)
    up = jnp.dot(a, w["w_up"], preferred_element_type=jnp.float32)
    return h + matmul((jax.nn.silu(gate) * up).astype(jnp.bfloat16), w["w_down"])


def adamw(w, m, v, g):
    m = 0.9 * m + 0.1 * g
    v = 0.95 * v + 0.05 * g * g
    step = m * lax.rsqrt(v + 1e-8) + 0.1 * w
    return (w - 0.02 * step).astype(jnp.bfloat16), m, v


def stack(weights, h):
    return lax.scan(lambda h, w: (layer(h, w), None), h, weights)[0]


def reference(x, dy, w_gate, w_up, w_down, m_w_gate, m_w_up, m_w_down, v_w_gate, v_w_up, v_w_down):
    weights = dict(zip(NAMES, (w_gate, w_up, w_down), strict=True))

    def take(so_far, sequence):
        h, by_y = sequence
        _, back = jax.vjp(lambda w: stack(w, h), weights)
        return jax.tree.map(lambda total, term: total + term.astype(jnp.float32), so_far, back(by_y)[0]), None

    none_yet = {name: jnp.zeros(w.shape, jnp.float32) for name, w in weights.items()}
    by_weights, _ = lax.scan(take, none_yet, (x, dy))
    gradients = [by_weights[name].astype(jnp.bfloat16).astype(jnp.float32) for name in NAMES]
    new = [
        adamw(w.astype(jnp.float32), m, v, g)
        for w, m, v, g in zip((w_gate, w_up, w_down), (m_w_gate, m_w_up, m_w_down), (v_w_gate, v_w_up, v_w_down), gradients, strict=True)
    ]
    return tuple(one[which] for which in range(3) for one in new)
```

```python
import jax
import jax.numpy as jnp
from jax import lax
from jax.experimental import pallas as pl
from jax.experimental.pallas import tpu as pltpu
from jax.sharding import PartitionSpec as P

NAMES = ("w_gate", "w_up", "w_down")
BF, F32 = jnp.bfloat16, jnp.float32
NN, NT, TN = ((((1,), (0,)), ((), ())), (((1,), (1,)), ((), ())), (((0,), (0,)), ((), ())))
MESH = pl.DeviceIdType.MESH
BN = 256


def mm(a, b, dims=NN):
    return lax.dot_general(a, b, dims, preferred_element_type=F32)


def whole(shape):
    return pl.BlockSpec(shape, lambda j: (0,) * len(shape), pipeline_mode=pl.Buffered(1))


def cols(rows, n):
    return pl.BlockSpec((rows, n), lambda j: (0, j))


def rows(m, columns):
    return pl.BlockSpec((m, columns), lambda j: (j, 0))


def sds(shape, dtype=BF):
    return jax.ShapeDtypeStruct(shape, dtype)


def normed(wide):
    return (wide * lax.rsqrt(jnp.mean(wide * wide, -1, keepdims=True) + 1e-6)).astype(BF)


class Place:
    def __init__(self, mesh):
        self.nx, self.ny = mesh.shape["s"] // 2, mesh.shape["r"]
        s = lax.axis_index("s")
        self.x, self.c, self.y = s // 2, s % 2, lax.axis_index("r")
        self.to = {
            "x+": {"s": (s + 2) % (2 * self.nx)},
            "x-": {"s": (s + 2 * self.nx - 2) % (2 * self.nx)},
            "y+": {"r": (self.y + 1) % self.ny},
            "y-": {"r": (self.y + self.ny - 1) % self.ny},
            "d": {"s": s + 1 - 2 * self.c},
        }

    def meet(self):
        barrier = pltpu.get_barrier_semaphore()
        for target in self.to.values():
            pl.semaphore_signal(barrier, inc=1, device_id=target, device_id_type=MESH)
        pl.semaphore_wait(barrier, len(self.to))


class Gather:
    def __init__(self, place, by, shard, full, stage, send, recv, local):
        self.p, self.by, self.shard, self.full, self.stage = place, by, shard, full, stage
        self.send, self.recv, self.local = send, recv, local
        self.n = shard.shape[0]
        self.stages = 3 if by == "x" else 5

    def span(self, x, start=0, size=None):
        p = self.p
        return pl.ds(pl.multiple_of((2 * (x % p.nx) + p.c) * self.n + start, 8), self.n if size is None else size)

    def copy(self, k, way, x, start=0, size=None, own=False):
        at = self.full.at[self.span(x, start, size)]
        src = at
        if own:
            src = self.shard.at[pl.ds(pl.multiple_of(start, 8) if size else 0, size or self.n)]
        return lambda: pltpu.make_async_remote_copy(
            src_ref=src, dst_ref=at, send_sem=self.send.at[k], recv_sem=self.recv.at[k], device_id=self.p.to[way], device_id_type=MESH
        )

    def copies(self):
        p, n, x = self.p, self.n, self.p.x
        k = iter(range(100))
        if self.by == "x":
            h = n // 2
            a = [self.copy(next(k), "x+", x, own=True), self.copy(next(k), "x-", x, own=True), self.copy(next(k), "d", x, own=True)]
            b = [
                self.copy(next(k), "x+", x + p.nx - 1, 0, h),
                self.copy(next(k), "x-", x + 1, h, n - h),
                self.copy(next(k), "d", x + p.nx - 1),
                self.copy(next(k), "d", x + 1),
            ]
            d = [self.copy(next(k), "d", x + 2)]
            return [([], a), (a[:2], b), (b[:2], d)], a[2:] + b[2:] + d, a + b + d
        q = n // 4
        h = (q // 2 + 7) // 8 * 8
        y, yp, ym = p.y * q, ((p.y + 1) % p.ny) * q, ((p.y + p.ny - 1) % p.ny) * q
        near = (x + p.nx - 1, x + 1)
        a = [self.copy(next(k), "x+", x, y, q, own=True), self.copy(next(k), "x-", x, y, q, own=True), self.copy(next(k), "d", x, own=True)]
        b = [self.copy(next(k), "x+", near[0], y, h), self.copy(next(k), "x-", near[1], y + h, q - h)]
        b += [self.copy(next(k), way, at, y, q) for at in near for way in ("y+", "y-")]
        c = [self.copy(next(k), way, x + 2, y, q) for way in ("y+", "y-")]
        every = (*near, x + 2)
        d = [self.copy(next(k), "y+", at, ym, h) for at in every] + [self.copy(next(k), "y-", at, yp + h, q - h) for at in every]
        e = [self.copy(next(k), "d", at) for at in every]
        return [([], a), (a[:2], b), (b[:2], c), (b[2:] + c, d), (d, e)], a[2:] + e, a + b + c + d + e

    def run(self, stage):
        stages, _, _ = self.copies()
        before, now = stages[stage]
        for one in before:
            one().wait_recv()
        for one in now:
            one().start()
        if stage == 0:
            pltpu.make_async_copy(self.shard, self.stage, self.local.at[0]).start()
        if stage == 1:
            pltpu.make_async_copy(self.shard, self.stage, self.local.at[0]).wait()
            pltpu.make_async_copy(self.stage, self.full.at[self.span(self.p.x)], self.local.at[1]).start()

    def finish(self):
        _, last, every = self.copies()
        for one in last:
            one().wait_recv()
        for one in every:
            one().wait_send()
        pltpu.make_async_copy(self.stage, self.full.at[self.span(self.p.x)], self.local.at[1]).wait()


def call(mesh, name, body, steps, args, in_specs, out_specs, out_shape, flops, gathers=(), plan=(), end=(), cid=None):
    n_in, n_out, n_g = len(args), len(out_specs), len(gathers)
    group = mesh.shape["s"]

    def kernel(*refs):
        ins, refs = refs[:n_in], refs[n_in:]
        shards, refs = refs[:n_g], refs[n_g:]
        outs, refs = refs[:n_out], refs[n_out:]
        fulls, refs = refs[:n_g], refs[n_g:]
        step = pl.program_id(0)
        if n_g:
            place = Place(mesh)
            items = [
                Gather(place, by, shard.at[layer], full, *refs[4 * i : 4 * i + 4])
                for i, ((_, layer, by), shard, full) in enumerate(zip(gathers, shards, fulls, strict=True))
            ]
            for at, todo in enumerate(plan):
                if todo:

                    @pl.when(step == at)
                    def _(at=at, todo=todo):
                        if at == 0:
                            place.meet()
                        for g, stage in todo:
                            items[g].run(stage)

        body(*ins, *outs)
        if n_g:

            @pl.when(step == steps - 1)
            def _():
                for g, stage in end:
                    items[g].run(stage)
                for item in items:
                    item.finish()

    hbm = pl.BlockSpec(memory_space=pltpu.HBM)
    scratch, fulls = [], []
    for shards, _, _ in gathers:
        _, n, columns = shards.shape
        fulls.append(sds((group * n, columns)))
        scratch += [pltpu.VMEM((n, columns), BF), pltpu.SemaphoreType.DMA((20,)), pltpu.SemaphoreType.DMA((20,)), pltpu.SemaphoreType.DMA((2,))]
    nbytes = sum(a.size * a.dtype.itemsize for a in args) + sum(o.size * jnp.dtype(o.dtype).itemsize for o in out_shape)
    return pl.pallas_call(
        kernel,
        grid=(steps,),
        in_specs=list(in_specs) + [hbm] * n_g,
        out_specs=list(out_specs) + [hbm] * n_g,
        out_shape=list(out_shape) + fulls,
        scratch_shapes=scratch,
        compiler_params=pltpu.CompilerParams(
            vmem_limit_bytes=60 * 2**20,
            dimension_semantics=("arbitrary",),
            **({"collective_id": cid, "has_side_effects": True} if n_g else {}),
        ),
        cost_estimate=pl.CostEstimate(flops=flops, bytes_accessed=nbytes, transcendentals=0),
        name=name,
    )(*args, *(g[0] for g in gathers))


def prepare(mesh, x, gathers, **kw):
    tokens, d = x.shape
    block = tokens // 4

    def body(x_ref, a_ref):
        a_ref[...] = normed(x_ref[...].astype(F32))

    return call(mesh, "prepare", body, 4, [x], [rows(block, d)], [rows(block, d)], [sds(x.shape)], x.size, gathers, **kw)


def gate_up(mesh, a, wg, wu, gathers, **kw):
    (tokens, d), f = a.shape, wg.shape[1]

    def body(a_ref, g_ref, u_ref, p_ref, go_ref, uo_ref):
        g, u = mm(a_ref[...], g_ref[...]), mm(a_ref[...], u_ref[...])
        go_ref[...], uo_ref[...] = g, u
        p_ref[...] = (g * jax.nn.sigmoid(g) * u).astype(BF)

    return call(
        mesh, "gate_up", body, f // BN, [a, wg, wu], [whole(a.shape), cols(d, BN), cols(d, BN)], [cols(tokens, BN)] * 3,
        [sds((tokens, f)), sds((tokens, f), F32), sds((tokens, f), F32)], 4 * tokens * d * f, gathers, **kw
    )


def down(mesh, h, p, wd, gathers, **kw):
    (tokens, d), f = h.shape, p.shape[1]
    block = tokens // 4

    def body(h_ref, p_ref, w_ref, ho_ref, a_ref):
        new = h_ref[...] + mm(p_ref[...], w_ref[...]).astype(BF)
        ho_ref[...] = new
        a_ref[...] = normed(new.astype(F32))

    return call(
        mesh, "down", body, 4, [h, p, wd], [rows(block, d), rows(block, f), whole(wd.shape)], [rows(block, d)] * 2,
        [sds(h.shape)] * 2, 2 * tokens * d * f, gathers, **kw
    )


def by_gate_up(by_p, g, u):
    s = jax.nn.sigmoid(g)
    silu = g * s
    return (by_p * u * (s * (1 + g * (1 - s)))).astype(BF), (by_p * silu).astype(BF), silu


def last_layer(mesh, a, dy, wg, wu, wd):
    (tokens, d), f = a.shape, wg.shape[1]

    def body(a_ref, y_ref, g_ref, u_ref, d_ref, p_ref, bg_ref, bu_ref):
        g, u = mm(a_ref[...], g_ref[...]), mm(a_ref[...], u_ref[...])
        by_p = mm(y_ref[...], d_ref[...], NT).astype(BF).astype(F32)
        bg_ref[...], bu_ref[...], silu = by_gate_up(by_p, g, u)
        p_ref[...] = (silu * u).astype(BF)

    return call(
        mesh, "last_layer", body, f // BN, [a, dy, wg, wu, wd], [whole(a.shape), whole(dy.shape), cols(d, BN), cols(d, BN), rows(BN, d)],
        [cols(tokens, BN)] * 3, [sds((tokens, f))] * 3, 6 * tokens * d * f
    )


def by_hidden(mesh, g, u, dy, wd):
    (tokens, d), f = dy.shape, wd.shape[0]

    def body(g_ref, u_ref, y_ref, d_ref, bg_ref, bu_ref):
        by_p = mm(y_ref[...], d_ref[...], NT).astype(BF).astype(F32)
        bg_ref[...], bu_ref[...], _ = by_gate_up(by_p, g_ref[...], u_ref[...])

    return call(
        mesh, "by_hidden", body, f // BN, [g, u, dy, wd], [cols(tokens, BN), cols(tokens, BN), whole(dy.shape), rows(BN, d)],
        [cols(tokens, BN)] * 2, [sds((tokens, f))] * 2, 2 * tokens * d * f
    )


def by_states(mesh, dy, h, bg, bu, wg, wu):
    (tokens, d), f = h.shape, bg.shape[1]
    block = tokens // 4

    def body(y_ref, h_ref, bg_ref, bu_ref, g_ref, u_ref, o_ref):
        by_a = (mm(bg_ref[...], g_ref[...], NT).astype(BF) + mm(bu_ref[...], u_ref[...], NT).astype(BF)).astype(F32)
        x = h_ref[...].astype(F32)
        scale = lax.rsqrt(jnp.mean(x * x, -1, keepdims=True) + 1e-6)
        along = jnp.mean(by_a * x, -1, keepdims=True)
        o_ref[...] = y_ref[...] + (by_a * scale - x * (scale * scale * scale * along)).astype(BF)

    return call(
        mesh, "by_states", body, 4, [dy, h, bg, bu, wg, wu],
        [rows(block, d), rows(block, d), rows(block, f), rows(block, f), whole(wg.shape), whole(wu.shape)],
        [rows(block, d)], [sds(h.shape)], 4 * tokens * d * f
    )[0]


def by_weight(mesh, left, right, name):
    (tokens, m), n = left.shape, right.shape[1]

    def body(l_ref, r_ref, o_ref):
        o_ref[...] = mm(l_ref[...], r_ref[...], TN).astype(BF)

    return call(mesh, name, body, m // BN, [left, right], [cols(tokens, BN), whole(right.shape)], [rows(BN, n)], [sds((m, n))], 2 * tokens * m * n)[0]


def adamw(w, m, v, g):
    m = 0.9 * m + 0.1 * g
    v = 0.95 * v + 0.05 * g * g
    step = m * lax.rsqrt(v + 1e-8) + 0.1 * w
    return (w - 0.02 * step).astype(BF), m, v


def solution(mesh):
    def summed(term):
        return lax.psum(lax.psum_scatter(term, "s", scatter_dimension=0, tiled=True), "r")

    def step(x, dy, *arrays):
        weights, m, v = (arrays[i : i + 3] for i in (0, 3, 6))
        wg, wu, wd = weights
        h0, dy = x[0], dy[0]
        a0, u0, g0 = prepare(mesh, h0, [(wu, 0, "y"), (wg, 0, "x")], plan=[[(0, 0)], [], [(0, 1), (1, 0)], []],
            end=[(0, 2), (0, 3), (1, 1), (0, 4), (1, 2)], cid=0)
        p0, zg0, zu0, d0, g1 = gate_up(mesh, a0, g0, u0, [(wd, 0, "x"), (wg, 1, "y")],
            plan=[[(1, 0)], [], [(1, 1), (0, 0)], [], [(1, 2)], [], [(1, 3)], [], [], [(0, 1), (1, 4)], []],
            end=[(0, 2)], cid=1)
        h1, a1, u1, d1 = down(mesh, h0, p0, d0, [(wu, 1, "y"), (wd, 1, "x")], plan=[[(0, 0)], [(0, 1), (1, 0)], [(0, 2)], [(0, 3)]],
            end=[(1, 1), (0, 4), (1, 2)], cid=2)
        p1, bg1, bu1 = last_layer(mesh, a1, dy, g1, u1, d1)
        terms = {}

        def term(name, left, right, then):
            terms[name], *then = lax.optimization_barrier((by_weight(mesh, left, right, name), *then))
            return then

        (a1,) = term("by_down_1", p1, dy, [a1])
        (a1, bg1) = term("by_gate_1", a1, bg1, [a1, bg1])
        bg1, bu1 = term("by_up_1", a1, bu1, [bg1, bu1])
        by_h = by_states(mesh, dy, h1, bg1, bu1, g1, u1)
        by_h, zg0 = term("by_down_0", p0, by_h, [by_h, zg0])
        bg0, bu0 = by_hidden(mesh, zg0, zu0, by_h, d0)
        (bu0,) = term("by_gate_0", a0, bg0, [bu0])
        term("by_up_0", a0, bu0, [])
        mine = [[summed(terms[f"by_{one}_{number}"]) for one in ("gate", "up", "down")] for number in range(2)]
        gradients = [jnp.stack([mine[number][i] for number in range(2)]).astype(F32) for i in range(3)]
        new = [adamw(w.astype(F32), m, v, g) for w, m, v, g in zip(weights, m, v, gradients, strict=True)]
        return tuple(one[which] for which in range(3) for one in new)

    states, cut = P(("rep", "r", "s"), None, None), P(None, "s", None)
    return jax.shard_map(
        step,
        mesh=mesh,
        in_specs=(states, states) + (cut,) * 9,
        out_specs=(P("rep", "s", None),) * 9,
        check_vma=False,
    )
```

```python
import jax
import jax.numpy as jnp
from jax import lax
from jax.experimental import pallas as pl
from jax.experimental.pallas import tpu as pltpu
from jax.sharding import PartitionSpec as P

NAMES = ("w_gate", "w_up", "w_down")
BF, F32 = jnp.bfloat16, jnp.float32
NN, NT, TN = ((((1,), (0,)), ((), ())), (((1,), (1,)), ((), ())), (((0,), (0,)), ((), ())))
MESH = pl.DeviceIdType.MESH
BN = 256


def mm(a, b, dims=NN):
    return lax.dot_general(a, b, dims, preferred_element_type=F32)


def whole(shape):
    return pl.BlockSpec(shape, lambda j: (0,) * len(shape), pipeline_mode=pl.Buffered(1))


def cols(rows, n):
    return pl.BlockSpec((rows, n), lambda j: (0, j))


def rows(m, columns):
    return pl.BlockSpec((m, columns), lambda j: (j, 0))


def sds(shape, dtype=BF):
    return jax.ShapeDtypeStruct(shape, dtype)


def normed(wide):
    return (wide * lax.rsqrt(jnp.mean(wide * wide, -1, keepdims=True) + 1e-6)).astype(BF)


class Place:
    def __init__(self, mesh):
        self.nx, self.ny = mesh.shape["s"] // 2, mesh.shape["r"]
        s = lax.axis_index("s")
        self.x, self.c, self.y = s // 2, s % 2, lax.axis_index("r")
        self.to = {
            "x+": {"s": (s + 2) % (2 * self.nx)},
            "x-": {"s": (s + 2 * self.nx - 2) % (2 * self.nx)},
            "y+": {"r": (self.y + 1) % self.ny},
            "y-": {"r": (self.y + self.ny - 1) % self.ny},
            "d": {"s": s + 1 - 2 * self.c},
        }

    def meet(self):
        barrier = pltpu.get_barrier_semaphore()
        for target in self.to.values():
            pl.semaphore_signal(barrier, inc=1, device_id=target, device_id_type=MESH)
        pl.semaphore_wait(barrier, len(self.to))


class Gather:
    def __init__(self, place, by, shard, full, stage, send, recv, local):
        self.p, self.by, self.shard, self.full, self.stage = place, by, shard, full, stage
        self.send, self.recv, self.local = send, recv, local
        self.n = shard.shape[0]

    def span(self, x, start=0, size=None):
        p = self.p
        return pl.ds(pl.multiple_of((2 * (x % p.nx) + p.c) * self.n + start, 8), self.n if size is None else size)

    def copy(self, k, way, x, start=0, size=None, own=False):
        at = self.full.at[self.span(x, start, size)]
        src = at
        if own:
            src = self.shard.at[pl.ds(pl.multiple_of(start, 8) if size else 0, size or self.n)]
        return lambda: pltpu.make_async_remote_copy(
            src_ref=src, dst_ref=at, send_sem=self.send.at[k], recv_sem=self.recv.at[k], device_id=self.p.to[way], device_id_type=MESH
        )

    def copies(self):
        p, n, x = self.p, self.n, self.p.x
        k = iter(range(100))
        if self.by == "x":
            h, west, east = n // 2, x + p.nx - 1, x + 1
            a = [self.copy(next(k), "x+", x, 0, h, own=True), self.copy(next(k), "x-", x, h, n - h, own=True), self.copy(next(k), "d", x, own=True)]
            b = [self.copy(next(k), "x+", x, h, n - h, own=True), self.copy(next(k), "x-", x, 0, h, own=True)]
            c = [self.copy(next(k), "x+", west, 0, h), self.copy(next(k), "x-", east, h, n - h)]
            d = [self.copy(next(k), "d", west), self.copy(next(k), "d", east)]
            e = [self.copy(next(k), "d", x + 2)]
            return [([], a), ([], b), (a[:2], c), (b, d), (c, e)], a[2:] + d + e, a + b + c + d + e
        q = n // 4
        h = (q // 2 + 7) // 8 * 8
        y, yp, ym = p.y * q, ((p.y + 1) % p.ny) * q, ((p.y + p.ny - 1) % p.ny) * q
        near = (x + p.nx - 1, x + 1)
        a = [self.copy(next(k), "x+", x, y, q, own=True), self.copy(next(k), "x-", x, y, q, own=True), self.copy(next(k), "d", x, own=True)]
        b = [self.copy(next(k), "x+", near[0], y, h), self.copy(next(k), "x-", near[1], y + h, q - h)]
        b += [self.copy(next(k), way, at, y, q) for at in near for way in ("y+", "y-")]
        c = [self.copy(next(k), way, x + 2, y, q) for way in ("y+", "y-")]
        every = (*near, x + 2)
        d = [self.copy(next(k), "y+", at, ym, h) for at in every] + [self.copy(next(k), "y-", at, yp + h, q - h) for at in every]
        e = [self.copy(next(k), "d", at) for at in every]
        return [([], a), (a[:2], b), (b[:2], c), (b[2:] + c, d), (d, e)], a[2:] + e, a + b + c + d + e

    def run(self, stage):
        stages, _, _ = self.copies()
        before, now = stages[stage]
        for one in before:
            one().wait_recv()
        for one in now:
            one().start()
        if stage == 0:
            pltpu.make_async_copy(self.shard, self.stage, self.local.at[0]).start()
        if stage == 1:
            pltpu.make_async_copy(self.shard, self.stage, self.local.at[0]).wait()
            pltpu.make_async_copy(self.stage, self.full.at[self.span(self.p.x)], self.local.at[1]).start()

    def finish(self):
        _, last, every = self.copies()
        for one in last:
            one().wait_recv()
        for one in every:
            one().wait_send()
        pltpu.make_async_copy(self.stage, self.full.at[self.span(self.p.x)], self.local.at[1]).wait()


class Exchange:
    def __init__(self, place, send, recv):
        self.p, self.send, self.recv = place, send, recv

    def copy(self, k, way, src, dst):
        return lambda: pltpu.make_async_remote_copy(
            src_ref=src, dst_ref=dst, send_sem=self.send.at[k], recv_sem=self.recv.at[k], device_id=self.p.to[way], device_id_type=MESH
        )

    def run(self, stage):
        before, now = self.stages[stage]
        for one in before:
            one().wait_recv()
        for one in now:
            one().start()

    def finish(self):
        waited = [one for before, _ in self.stages for one in before]
        every = [one for _, now in self.stages for one in now]
        for one in every:
            if one not in waited:
                one().wait_recv()
        for one in every:
            one().wait_send()


class Beside(Exchange):
    def __init__(self, place, mine, theirs, send, recv):
        super().__init__(place, send, recv)
        h = mine.shape[0] // 2
        top, bottom = pl.ds(0, h), pl.ds(h, mine.shape[0] - h)
        a = [self.copy(0, "y+", mine, theirs.at[0]), self.copy(1, "y-", mine, theirs.at[1])]
        b = [self.copy(2, "y+", theirs.at[0, top], theirs.at[2, top]), self.copy(3, "y-", theirs.at[1, bottom], theirs.at[2, bottom])]
        self.stages = [([], a), (a, b)]


def sems(n):
    return [pltpu.SemaphoreType.DMA((n,)), pltpu.SemaphoreType.DMA((n,))]


def gather(mesh, shards, layer, by):
    _, n, columns = shards.shape
    scratch = [pltpu.VMEM((n, columns), BF), *sems(20), pltpu.SemaphoreType.DMA((2,))]
    make = lambda place, ins, outs, scr: Gather(place, by, ins[0].at[layer], outs[0], *scr)
    return shards, [sds((mesh.shape["s"] * n, columns))], scratch, make


def beside(mine):
    return mine, [sds((3, *mine.shape))], sems(4), lambda place, ins, outs, scr: Beside(place, *ins, *outs, *scr)


def split(refs, sizes):
    out, at = [], 0
    for size in sizes:
        out.append(refs[at : at + size])
        at += size
    return out


def call(mesh, name, body, steps, args, in_specs, out_specs, out_shape, flops, items=(), plan=(), end=(), cid=None):
    n_in, n_out, n_i = len(args), len(out_specs), len(items)
    extra = [out for item in items for out in item[1]]
    scratch = [one for item in items for one in item[2]]

    def kernel(*refs):
        ins, sources, outs, dests, scr = split(refs, [n_in, n_i, n_out, len(extra), len(scratch)])
        step = pl.program_id(0)
        made = []
        if n_i:
            place = Place(mesh)
            parts = zip(items, sources, split(dests, [len(i[1]) for i in items]), split(scr, [len(i[2]) for i in items]), strict=True)
            made = [item[3](place, [source], dest, own) for item, source, dest, own in parts]
            for at, todo in enumerate(plan):
                if todo:

                    @pl.when(step == at)
                    def _(at=at, todo=todo):
                        if at == 0:
                            place.meet()
                        for i, stage in todo:
                            made[i].run(stage)

        body(*ins, *outs)
        if n_i:

            @pl.when(step == steps - 1)
            def _():
                for i, stage in end:
                    made[i].run(stage)
                for one in made:
                    one.finish()

    hbm = pl.BlockSpec(memory_space=pltpu.HBM)
    nbytes = sum(a.size * a.dtype.itemsize for a in args) + sum(o.size * jnp.dtype(o.dtype).itemsize for o in out_shape)
    return pl.pallas_call(
        kernel,
        grid=(steps,),
        in_specs=list(in_specs) + [hbm] * n_i,
        out_specs=list(out_specs) + [hbm] * len(extra),
        out_shape=list(out_shape) + extra,
        scratch_shapes=scratch,
        compiler_params=pltpu.CompilerParams(
            vmem_limit_bytes=60 * 2**20,
            dimension_semantics=("arbitrary",),
            **({"collective_id": cid, "has_side_effects": True} if n_i else {}),
        ),
        cost_estimate=pl.CostEstimate(flops=flops, bytes_accessed=nbytes, transcendentals=0),
        name=name,
    )(*args, *(item[0] for item in items))


def prepare(mesh, x, items=(), **kw):
    tokens, d = x.shape
    block = tokens // 4

    def body(x_ref, a_ref):
        a_ref[...] = normed(x_ref[...].astype(F32))

    return call(mesh, "prepare", body, 4, [x], [rows(block, d)], [rows(block, d)], [sds(x.shape)], x.size, items, **kw)


def gate_up(mesh, a, wg, wu, items=(), **kw):
    (tokens, d), f = a.shape, wg.shape[1]

    def body(a_ref, g_ref, u_ref, p_ref, go_ref, uo_ref):
        g, u = mm(a_ref[...], g_ref[...]), mm(a_ref[...], u_ref[...])
        go_ref[...], uo_ref[...] = g, u
        p_ref[...] = (g * jax.nn.sigmoid(g) * u).astype(BF)

    return call(
        mesh, "gate_up", body, f // BN, [a, wg, wu], [whole(a.shape), cols(d, BN), cols(d, BN)], [cols(tokens, BN)] * 3,
        [sds((tokens, f)), sds((tokens, f), F32), sds((tokens, f), F32)], 4 * tokens * d * f, items, **kw
    )


def down(mesh, h, p, wd, items=(), **kw):
    (tokens, d), f = h.shape, p.shape[1]
    block = tokens // 4

    def body(h_ref, p_ref, w_ref, ho_ref, a_ref):
        new = h_ref[...] + mm(p_ref[...], w_ref[...]).astype(BF)
        ho_ref[...] = new
        a_ref[...] = normed(new.astype(F32))

    return call(
        mesh, "down", body, 4, [h, p, wd], [rows(block, d), rows(block, f), whole(wd.shape)], [rows(block, d)] * 2,
        [sds(h.shape)] * 2, 2 * tokens * d * f, items, **kw
    )


def by_gate_up(by_p, g, u):
    s = jax.nn.sigmoid(g)
    silu = g * s
    return (by_p * u * (s * (1 + g * (1 - s)))).astype(BF), (by_p * silu).astype(BF), silu


def last_layer(mesh, a, dy, wg, wu, wd):
    (tokens, d), f = a.shape, wg.shape[1]

    def body(a_ref, y_ref, g_ref, u_ref, d_ref, p_ref, bg_ref, bu_ref):
        g, u = mm(a_ref[...], g_ref[...]), mm(a_ref[...], u_ref[...])
        by_p = mm(y_ref[...], d_ref[...], NT).astype(BF).astype(F32)
        bg_ref[...], bu_ref[...], silu = by_gate_up(by_p, g, u)
        p_ref[...] = (silu * u).astype(BF)

    return call(
        mesh, "last_layer", body, f // BN, [a, dy, wg, wu, wd], [whole(a.shape), whole(dy.shape), cols(d, BN), cols(d, BN), rows(BN, d)],
        [cols(tokens, BN)] * 3, [sds((tokens, f))] * 3, 6 * tokens * d * f
    )


def by_hidden(mesh, g, u, dy, wd, items=(), **kw):
    (tokens, d), f = dy.shape, wd.shape[0]

    def body(g_ref, u_ref, y_ref, d_ref, bg_ref, bu_ref):
        by_p = mm(y_ref[...], d_ref[...], NT).astype(BF).astype(F32)
        bg_ref[...], bu_ref[...], _ = by_gate_up(by_p, g_ref[...], u_ref[...])

    return call(
        mesh, "by_hidden", body, f // BN, [g, u, dy, wd], [cols(tokens, BN), cols(tokens, BN), whole(dy.shape), rows(BN, d)],
        [cols(tokens, BN)] * 2, [sds((tokens, f))] * 2, 2 * tokens * d * f, items, **kw
    )


def by_states(mesh, dy, h, bg, bu, wg, wu, items=(), **kw):
    (tokens, d), f = h.shape, bg.shape[1]
    block = tokens // 4

    def body(y_ref, h_ref, bg_ref, bu_ref, g_ref, u_ref, o_ref):
        by_a = (mm(bg_ref[...], g_ref[...], NT).astype(BF) + mm(bu_ref[...], u_ref[...], NT).astype(BF)).astype(F32)
        x = h_ref[...].astype(F32)
        scale = lax.rsqrt(jnp.mean(x * x, -1, keepdims=True) + 1e-6)
        along = jnp.mean(by_a * x, -1, keepdims=True)
        o_ref[...] = y_ref[...] + (by_a * scale - x * (scale * scale * scale * along)).astype(BF)

    return call(
        mesh, "by_states", body, 4, [dy, h, bg, bu, wg, wu],
        [rows(block, d), rows(block, d), rows(block, f), rows(block, f), whole(wg.shape), whole(wu.shape)],
        [rows(block, d)], [sds(h.shape)], 4 * tokens * d * f, items, **kw
    )


def by_weight(mesh, left, right, name, items=(), **kw):
    (tokens, m), n = left.shape, right.shape[1]

    def body(l_ref, r_ref, o_ref):
        o_ref[...] = mm(l_ref[...], r_ref[...], TN).astype(BF)

    return call(mesh, name, body, m // BN, [left, right], [cols(tokens, BN), whole(right.shape)], [rows(BN, n)], [sds((m, n))], 2 * tokens * m * n, items, **kw)


def by_weights(mesh, lefts, rights, cid):
    (tokens, m), n, many = lefts[0].shape, rights[0].shape[1], len(rights)
    nx, ny = mesh.shape["s"] // 2, mesh.shape["r"]
    block, own = m // nx, m // (2 * nx)
    half, steps = own // 2, many * nx
    part = own // ny
    piece = part // 2
    away = (2, 1, nx - 1, 0)

    def kernel(l0_ref, l1_ref, r0_hbm, r1_hbm, r2_hbm, o_ref, rhs_ref, t_ref, r_ref, h_ref, x_ref, y_ref, a_ref, b_ref, g_ref, s_sem, send, recv):
        step = pl.program_id(0)
        place = Place(mesh)
        mine = pl.ds(pl.multiple_of(place.c * own, 8), own)
        other = pl.ds(pl.multiple_of((1 - place.c) * own, 8), own)
        top, bottom = pl.ds(0, half), pl.ds(half, own - half)

        def copy(k, way, src, dst):
            return pltpu.make_async_remote_copy(
                src_ref=src, dst_ref=dst, send_sem=send.at[k], recv_sem=recv.at[k], device_id=place.to[way], device_id_type=MESH
            )

        def swap(i):
            return copy(i, "d", t_ref.at[i % 3, other], r_ref.at[i])

        def far(w, up):
            part = top if up else bottom
            return copy(12 + 2 * w + up, "x+" if up else "x-", r_ref.at[4 * w, part], h_ref.at[w, 1 - up])

        def near(w, up):
            return copy(18 + 2 * w + up, "x+" if up else "x-", r_ref.at[4 * w + (1 if up else 2)], x_ref.at[w, 1 - up])

        def at(quarter, up=None):
            start = lax.rem(place.y + quarter, ny) * part
            return pl.ds(pl.multiple_of(start + (piece if up == 0 else 0), 16), part if up is None else piece)

        def y_far(w, up):
            return copy(24 + 2 * w + up, "y+" if up else "y-", y_ref.at[w, at(2, up)], a_ref.at[w, 1 - up])

        def y_near(w, up):
            return copy(30 + 2 * w + up, "y+" if up else "y-", y_ref.at[w, at(1 if up else ny - 1)], b_ref.at[w, 1 - up])

        def y_back(w, up):
            return copy(36 + 2 * w + up, "y+" if up else "y-", g_ref.at[w, at(0)], g_ref.at[w, at(0)])

        def y_across(w, up):
            rows_ = at(ny - 1 if up else 1, up)
            return copy(42 + 2 * w + up, "y+" if up else "y-", g_ref.at[w, rows_], g_ref.at[w, rows_])

        def add_swapped(i):
            swap(i).wait()
            r_ref[i] = (r_ref[i].astype(F32) + t_ref[i % 3, mine].astype(F32)).astype(BF)

        def add_far(w):
            far(w, 1).wait_recv()
            r_ref[4 * w + 1, top] = (r_ref[4 * w + 1, top].astype(F32) + h_ref[w, 0].astype(F32)).astype(BF)
            far(w, 0).wait_recv()
            r_ref[4 * w + 2, bottom] = (r_ref[4 * w + 2, bottom].astype(F32) + h_ref[w, 1].astype(F32)).astype(BF)

        def start(make, w):
            make(w, 1).start()
            make(w, 0).start()

        def add_near(w):
            near(w, 1).wait_recv()
            near(w, 0).wait_recv()
            total = r_ref[4 * w + 3].astype(F32) + (x_ref[w, 0].astype(F32) + x_ref[w, 1].astype(F32))
            y_ref[w] = total.astype(BF)

        def add_y_far(w):
            y_far(w, 1).wait()
            y_far(w, 0).wait()
            up, down_ = at(1, 1), at(ny - 1, 0)
            y_ref[w, up] = (y_ref[w, up].astype(F32) + a_ref[w, 0].astype(F32)).astype(BF)
            y_ref[w, down_] = (y_ref[w, down_].astype(F32) + a_ref[w, 1].astype(F32)).astype(BF)

        def add_y_near(w):
            y_near(w, 1).wait()
            y_near(w, 0).wait()
            whole_sum = y_ref[w, at(0)].astype(F32) + (b_ref[w, 0].astype(F32) + b_ref[w, 1].astype(F32))
            g_ref[w, at(0)] = whole_sum.astype(BF)

        def pass_on(w):
            y_back(w, 1).wait()
            y_back(w, 0).wait()
            start(y_across, w)

        def put(w):
            y_across(w, 1).wait()
            y_across(w, 0).wait()
            o_ref[w] = g_ref[w]

        load = [pltpu.make_async_copy(r, rhs_ref.at[w % 2], s_sem.at[w]) for w, r in enumerate((r0_hbm, r1_hbm, r2_hbm))]
        for now in range(steps):

            @pl.when(step == now)
            def _(now=now):
                if now == 0:
                    load[0].start()
                    load[1].start()
                    place.meet()
                    load[0].wait()
                if now == nx:
                    load[2].start()
                    load[1].wait()
                if now == 2 * nx:
                    load[2].wait()
                if now >= 1:
                    swap(now - 1).start()
                if now >= 2:
                    add_swapped(now - 2)
                if now == 5:
                    add_far(0)
                if now == 6:
                    start(near, 0)
                if now % nx == 3:
                    start(far, now // nx)
                if now == 10:
                    add_near(0)
                if now == 11:
                    start(y_far, 0)

        k = lax.rem(step, nx)
        shift = jnp.where(k == 0, away[0], jnp.where(k == 1, away[1], jnp.where(k == 2, away[2], away[3])))
        columns = pl.ds(pl.multiple_of(lax.rem(place.x + shift, nx) * block, block), block)
        slot = lax.rem(step, 3)
        for w, (l_ref, buffer) in enumerate(((l0_ref, 0), (l1_ref, 1), (l1_ref, 0))):

            @pl.when((step >= w * nx) & (step < (w + 1) * nx))
            def _(l_ref=l_ref, buffer=buffer):
                t_ref[slot] = mm(l_ref[:, columns], rhs_ref[buffer], TN).astype(BF)

        @pl.when(step == steps - 1)
        def _():
            add_swapped(10)
            swap(11).start()
            add_far(1)
            add_y_far(0)
            start(near, 1)
            start(y_near, 0)
            add_swapped(11)
            add_far(2)
            add_y_near(0)
            start(near, 2)
            start(y_back, 0)
            pass_on(0)
            add_near(1)
            put(0)
            start(y_far, 1)
            add_y_far(1)
            start(y_near, 1)
            add_y_near(1)
            start(y_back, 1)
            pass_on(1)
            add_near(2)
            put(1)
            start(y_far, 2)
            add_y_far(2)
            start(y_near, 2)
            add_y_near(2)
            start(y_back, 2)
            pass_on(2)
            put(2)
            for w in range(many):
                for make in (far, near):
                    make(w, 1).wait_send()
                    make(w, 0).wait_send()

    hbm = pl.BlockSpec(memory_space=pltpu.HBM)
    return pl.pallas_call(
        kernel,
        grid=(steps,),
        in_specs=[whole(lefts[0].shape)] * 2 + [hbm] * many,
        out_specs=whole((many, own, n)),
        out_shape=sds((many, own, n)),
        scratch_shapes=[
            pltpu.VMEM((2, *rights[0].shape), BF),
            pltpu.VMEM((3, block, n), BF),
            pltpu.VMEM((many * nx, own, n), BF),
            pltpu.VMEM((many, 2, half, n), BF),
            pltpu.VMEM((many, 2, own, n), BF),
            pltpu.VMEM((many, own, n), BF),
            pltpu.VMEM((many, 2, piece, n), BF),
            pltpu.VMEM((many, 2, part, n), BF),
            pltpu.VMEM((many, own, n), BF),
            pltpu.SemaphoreType.DMA((many,)),
            *sems(48),
        ],
        compiler_params=pltpu.CompilerParams(
            vmem_limit_bytes=63 * 2**20, dimension_semantics=("arbitrary",), collective_id=cid, has_side_effects=True
        ),
        cost_estimate=pl.CostEstimate(flops=12 * tokens * m * n, bytes_accessed=6 * tokens * n, transcendentals=0),
        name="by_weights",
    )(*lefts, *rights)


def adamw(w, m, v, g):
    m = 0.9 * m + 0.1 * g
    v = 0.95 * v + 0.05 * g * g
    step = m * lax.rsqrt(v + 1e-8) + 0.1 * w
    return (w - 0.02 * step).astype(BF), m, v


def solution(mesh):
    def summed(term):
        return lax.psum(lax.psum_scatter(term, "s", scatter_dimension=0, tiled=True), "r")

    def step(x, dy, *arrays):
        weights, m, v = (arrays[i : i + 3] for i in (0, 3, 6))
        wg, wu, wd = weights
        h0, dy = x[0], dy[0]
        keep = lax.optimization_barrier
        a0, u0, g0 = prepare(mesh, h0, [gather(mesh, wu, 0, "y"), gather(mesh, wg, 0, "x")], plan=[[(0, 0), (1, 0)], [], [(0, 1), (1, 1)], []],
            end=[(0, 2), (1, 2), (0, 3), (1, 3), (0, 4), (1, 4)], cid=0)
        p0, zg0, zu0, d0, g1 = gate_up(mesh, a0, g0, u0, [gather(mesh, wd, 0, "x"), gather(mesh, wg, 1, "y")],
            plan=[[(1, 0), (0, 0)], [], [(1, 1), (0, 1)], [], [(1, 2)], [(0, 2)], [], [(1, 3)], [], [(0, 3)], [(1, 4)]],
            end=[(0, 4)], cid=1)
        h1, a1, u1, d1 = down(mesh, h0, p0, d0, [gather(mesh, wu, 1, "y"), gather(mesh, wd, 1, "x")],
            plan=[[(0, 0), (1, 0)], [(0, 1), (1, 1)], [(0, 2)], [(1, 2)]], end=[(0, 3), (1, 3), (0, 4), (1, 4)], cid=2)
        p1, bg1, bu1 = last_layer(mesh, a1, dy, g1, u1, d1)

        def scattered(term):
            return lax.psum_scatter(term, "s", scatter_dimension=0, tiled=True)

        def total(mine, theirs):
            mine, theirs = mine.astype(F32), theirs.astype(F32)
            return ((mine + theirs[2]) + (theirs[0] + theirs[1])).astype(BF)

        by_down, a1 = keep((*by_weight(mesh, p1, dy, "by_down_1"), a1))
        down_1 = scattered(by_down)
        by_gate, a1, bg1 = keep((*by_weight(mesh, a1, bg1, "by_gate_1"), a1, bg1))
        gate_1 = scattered(by_gate)
        (by_h,) = by_states(mesh, dy, h1, bg1, bu1, g1, u1)
        down_1, by_h = keep((down_1, by_h))
        by_down, by_h, zg0 = keep((*by_weight(mesh, p0, by_h, "by_down_0"), by_h, zg0))
        down_0 = scattered(by_down)
        bg0, bu0, down_1_y = by_hidden(mesh, zg0, zu0, by_h, d0, [beside(down_1)], plan=[[(0, 0)], [], [], [], [], [], [], [(0, 1)], [], [], []], cid=4)
        gate_1, down_0, bg0 = keep((gate_1, down_0, bg0))
        gate_1, down_0 = lax.psum(gate_1, "r"), lax.psum(down_0, "r")
        three = by_weights(mesh, [a1, a0], [bu1, bg0, bu0], cid=3)
        mine = [[three[1], three[2], down_0], [gate_1, three[0], total(down_1, down_1_y)]]
        gradients = [jnp.stack([mine[number][i] for number in range(2)]).astype(F32) for i in range(3)]
        new = [adamw(w.astype(F32), m, v, g) for w, m, v, g in zip(weights, m, v, gradients, strict=True)]
        return tuple(one[which] for which in range(3) for one in new)

    states, cut = P(("rep", "r", "s"), None, None), P(None, "s", None)
    return jax.shard_map(
        step,
        mesh=mesh,
        in_specs=(states, states) + (cut,) * 9,
        out_specs=(P("rep", "s", None),) * 9,
        check_vma=False,
    )
```
